32 devices in a mesh: gx: 8 (over z, x), gy: 4 (over y, core).
Axes of the slice: x: 2, y: 2, z: 4, core: 2. Of those that a mesh axis runs over, the one named last changes fastest.
Arguments:
- velocity: float32 [3, 8192, 512], P(None, ('gx', 'gy')), may hold values from -6 to 6
- positions: float32 [3, 1024, 256], P(None, ('gx', 'gy')), may hold values from -6 to 6
- stiff_h: float32 [1024, 256], P(('gx', 'gy')), may hold values from 0.1 to 1
- stiff_v: float32 [1024, 256], P(('gx', 'gy')), may hold values from 0.1 to 1
- marker_owner: int32 [262144, 1], P(('gx', 'gy')), may hold values from 0 to 31; in each aligned block of 8192 rows (0 to 8191, 8192 to 16383, ...) at most 384 rows name the same one
- marker_element: int32 [262144], P(('gx', 'gy')), may hold values from 0 to 255
- marker_coords: float32 [3, 262144], P(None, ('gx', 'gy')), may hold values from -1 to 1
Outputs:
- new_positions: float32 [3, 1024, 256], P(None, ('gx', 'gy'))
- node_forces: float32 [3, 8192, 512], P(None, ('gx', 'gy'))
The draws below stay inside these ranges and needn't reach their ends.
Inputs may be any that keep to these rules, and one draw needn't show every extreme that they name: `marker_owner`: among the markers of one device's rows, no owner is named more than 384 times, and in some devices' rows one owner is named exactly 384 times.
All inputs are finite; a program needn't handle non-finite values.
Results may differ from the reference program's by a relative error of at most 0.00013.
Values sent between devices are 32-bit elements; how exact they have to be, the bound alone decides.
No kernel may reach another device: no remote copies, remote signals or barrier semaphores. Data moves between devices by JAX's collectives and lax.ppermute only.
A program may use at most 64 MiB of HBM per device.

```python
import math
import jax
import jax.numpy as jnp
import numpy as np
from jax import lax

POINTS = 8
NODES = 512
E_DEV = 256
ELEMS = 8192
COLS = 256
M_DEV = 8192
ROWS = 1024
MARKERS = 262144
CAP = 384
DEVICES = 32


def plant(drawn, own_key, low, high):
    dims = drawn.shape
    place = [jax.random.randint(jax.random.fold_in(own_key, axis), (), 0, dims[axis]) for axis in range(len(dims))]
    drawn = drawn.at[tuple(place)].set(low)
    longest = dims.index(max(dims))
    place[longest] = (place[longest] + 1) % dims[longest]
    return drawn.at[tuple(place)].set(high)


def levels(stream_key, shape, split, smallest, top_value):
    def one(axis_at, blocks):
        heights = jax.random.uniform(jax.random.fold_in(jax.random.fold_in(stream_key, 6), axis_at), (blocks,), jnp.float32, smallest / len(split), top_value / len(split))
        return jnp.repeat(jnp.exp(heights), shape[axis_at] // blocks).reshape((-1,) + (1,) * (len(shape) - axis_at - 1))

    level = one(*split[0])
    for cut in split[1:]:
        level = level * one(*cut)
    return level


def assign_block(rng, own, number, rows, amount, top, bound, slope):
    order = jax.random.permutation(rng, amount)
    heavy_load, usual = shares(amount, rows * top, bound, slope, True), shares(amount, rows * top, bound, slope, False)
    places = jnp.arange(amount)

    def named(tallies, rotation):
        used = int((tallies > 0).sum())
        fixed = max(1, used // 4)
        moved = fixed + (places - fixed + rotation * (used - fixed)) % max(1, amount - fixed)
        return jnp.zeros((amount,), jnp.int32).at[order[jnp.where(places < fixed, places, moved)]].set(jnp.asarray(tallies, jnp.int32))

    tallies = jnp.where(number % 4 == 0, named(heavy_load, number // 4), named(usual, number - number // 4 - 1))
    mixed = jax.random.permutation(jax.random.fold_in(own, 3), amount)
    giver, taker = mixed[0:amount // 2 * 2:2], mixed[1:amount // 2 * 2:2]
    slack = jnp.minimum(tallies[giver] - 1, bound - tallies[taker]) // 2
    slack = jnp.where((giver == order[0]) | (taker == order[0]) | (tallies[taker] == 0), 0, jnp.maximum(slack, 0))
    moved = jax.random.randint(jax.random.fold_in(own, 4), (amount // 2,), 0, 1 << 20) % (slack + 1)
    tallies = tallies.at[giver].add(-moved).at[taker].add(moved)
    labels = jnp.searchsorted(jnp.cumsum(tallies), jnp.arange(rows * top), side="right").astype(jnp.int32)
    table = labels.reshape(top, rows).T
    table = table[jax.random.permutation(jax.random.fold_in(own, 1), rows)]
    rotation = jax.random.randint(jax.random.fold_in(own, 2), (rows, 1), 0, top)
    return jnp.take_along_axis(table, (jnp.arange(top)[None, :] + rotation) % top, axis=1)


def shares(amount, total, reach, lean, full):
    weights = [(1 << 20) // math.isqrt(grade ** lean) + 1 for grade in range(1, amount + 1)]
    largest = reach if full else min(reach, max(-(-total // amount), total * weights[0] // sum(weights)))
    least = 1 if total - largest >= amount - 1 else 0
    counts, rest = [largest] + [least] * (amount - 1), total - largest - least * (amount - 1)
    while rest > 0:
        candidates = [i for i in range(1, amount) if counts[i] < largest] or [i for i in range(1, amount) if counts[i] < reach]
        whole, left = sum([weights[i] for i in candidates]), rest
        for i in candidates:
            extra = min(reach - counts[i], max(1, left * weights[i] // whole), rest)
            counts[i] = counts[i] + extra
            rest = rest - extra
    return np.array(counts)


def gaussian(own_key, shape, deviation, most, pieces=(), kind=jnp.bfloat16):
    drawn = jax.random.normal(own_key, shape, jnp.float32) * deviation
    if len(pieces) > 0:
        drawn = levels(own_key, shape, pieces, -0.22, 0.18) * drawn
    return jnp.clip(drawn, min=-most, max=most).astype(kind)


def setup_inputs(seed: int = 0) -> dict:
    seeds = jax.random.split(jax.random.key(seed), 8)
    velocity = gaussian(seeds[0], (3, ELEMS, NODES), 1.0, 6.0, ((1, 32),), jnp.float32)
    positions = gaussian(seeds[1], (3, ROWS, COLS), 1.0, 6.0, ((1, 32),), jnp.float32)
    stiff_h = jnp.clip(jnp.exp(math.log(1.0) - 2.3025851 * jax.random.uniform(seeds[2], (ROWS, COLS), jnp.float32) ** levels(seeds[2], (ROWS, COLS), ((0, 32),), -0.2, 0.2)), 0.1, 1.0)
    stiff_v = jnp.clip(jnp.exp(math.log(1.0) - 2.3025851 * jax.random.uniform(seeds[3], (ROWS, COLS), jnp.float32) ** levels(seeds[3], (ROWS, COLS), ((0, 32),), -0.2, 0.2)), 0.1, 1.0)
    marker_owner_keys = jax.random.split(jax.random.fold_in(seeds[4], 1), MARKERS // M_DEV)
    marker_owner_turns = jax.random.permutation(jax.random.fold_in(seeds[4], 3), MARKERS // M_DEV)
    marker_owner = jax.vmap(lambda own, number: assign_block(jax.random.fold_in(seeds[4], 2), own, number, M_DEV, DEVICES, 1, CAP, 2))(marker_owner_keys, marker_owner_turns).reshape((MARKERS, 1))
    marker_element = plant(jax.random.randint(seeds[5], (MARKERS,), 0, E_DEV), jax.random.fold_in(seeds[5], 1), 0, E_DEV - 1).astype(jnp.int32)
    marker_coords = jnp.clip(jax.random.uniform(seeds[6], (3, MARKERS), jnp.float32, -1.0, 1.0) * levels(seeds[6], (3, MARKERS), ((1, 32),), -0.4, 0.0), -1.0, 1.0)
    return {"velocity": velocity, "positions": positions, "stiff_h": stiff_h, "stiff_v": stiff_v, "marker_owner": marker_owner, "marker_element": marker_element, "marker_coords": marker_coords}


bend_modulus = 0.05
time_step = 0.5


def basis(values):
    abscissa = -jnp.cos(jnp.pi * jnp.arange(POINTS).astype(values.dtype) / (POINTS - 1))
    collected = []
    for i in range(POINTS):
        product = jnp.ones_like(values)
        for j in range(POINTS):
            if j != i:
                product = product * ((values - abscissa[j]) / (abscissa[i] - abscissa[j]))
        collected.append(product)
    return jnp.stack(collected)


def weight_table(factors):
    along_r = factors[0:POINTS].T
    along_s = factors[POINTS:2 * POINTS].T
    along_t = factors[2 * POINTS:3 * POINTS].T
    table = along_r[:, :, None, None] * along_s[:, None, :, None] * along_t[:, None, None, :]
    return table.reshape(along_r.shape[0], POINTS * POINTS * POINTS)


def surface_laplacian(extended):
    middle = extended[:, 1:-1]
    return extended[:, 2:] + extended[:, :-2] + jnp.roll(middle, 1, axis=2) + jnp.roll(middle, -1, axis=2) - 4.0 * middle


def tension(extended, stiff_h):
    points = extended[:3]
    vertical = extended[3]
    middle = points[:, 1:-1]
    return (stiff_h * (jnp.roll(middle, -1, axis=2) - middle)
            + jnp.roll(stiff_h, 1, axis=1) * (jnp.roll(middle, 1, axis=2) - middle)
            + vertical[1:-1] * (points[:, 2:] - middle)
            + vertical[:-2] * (points[:, :-2] - middle))


def wrap_rows(array):
    return jnp.concatenate([array[:, -1:], array, array[:, :1]], axis=1)


def reference(velocity, positions, stiff_h, stiff_v, marker_owner, marker_element, marker_coords):
    stacked = jnp.concatenate([positions, stiff_v[None]], axis=0)
    extended = wrap_rows(stacked)
    pulling = tension(extended, stiff_h)
    laplace = surface_laplacian(extended[:3])
    bending = -bend_modulus * surface_laplacian(wrap_rows(laplace))
    marker_force = (pulling + bending).reshape(3, MARKERS)
    element_ids = (marker_owner[:, 0] * E_DEV + marker_element).astype(jnp.int32)
    factors = jnp.concatenate([basis(marker_coords[0]), basis(marker_coords[1]), basis(marker_coords[2])], axis=0)
    factor_blocks = factors.reshape(3 * POINTS, DEVICES, M_DEV).transpose(1, 0, 2)
    element_blocks = element_ids.reshape(DEVICES, M_DEV)
    force_blocks = marker_force.reshape(3, DEVICES, M_DEV).transpose(1, 0, 2)

    def advance(running, inputs):
        block_factors, block_elements, pushes = inputs
        weights = weight_table(block_factors)
        gathered = jnp.take(velocity, block_elements, axis=1)
        sampled = jnp.sum(gathered * weights[None], axis=-1)
        running = running.at[:, block_elements, :].add(pushes[:, :, None] * weights[None])
        return running, sampled

    node_forces, sampled = lax.scan(advance, jnp.zeros_like(velocity), (factor_blocks, element_blocks, force_blocks))
    moved = sampled.transpose(1, 0, 2).reshape(3, ROWS, COLS)
    return positions + time_step * moved, node_forces
```

```python
import math

import jax
import jax.numpy as jnp
import numpy as np
from jax import lax
from jax.experimental import pallas as pl
from jax.experimental.pallas import tpu as pltpu
from jax.sharding import PartitionSpec as P

POINTS = 8
NODES = POINTS * POINTS * POINTS
AXES = ("gx", "gy")
LANES = 256
GROUP = 32

bend_modulus = 0.05
time_step = 0.5

ABSCISSA = -np.cos(np.pi * np.arange(POINTS) / (POINTS - 1))
SCALE = np.array(
    [1.0 / np.prod([ABSCISSA[i] - ABSCISSA[j] for j in range(POINTS) if j != i]) for i in range(POINTS)]
)

NN = (((1,), (0,)), ((), ()))
NT = (((1,), (1,)), ((), ()))


def dot(a, b, dims):
    return lax.dot_general(a, b, dims, preferred_element_type=jnp.float32)


def split(x):
    high = x.astype(jnp.bfloat16).astype(jnp.float32)
    return high, x - high


def sublane(shape):
    return lax.broadcasted_iota(jnp.int32, shape, 0)


def halo(positions, stiff_v):
    count = lax.axis_size(AXES)
    tail = jnp.concatenate(
        [positions[:, -2], positions[:, -1], stiff_v[-1:]], axis=0
    )
    head = jnp.concatenate([positions[:, 0], positions[:, 1]], axis=0)
    above = lax.ppermute(tail, AXES, [(i, (i + 1) % count) for i in range(count)])
    below = lax.ppermute(head, AXES, [((i + 1) % count, i) for i in range(count)])
    wide = jnp.concatenate(
        [above[0:3][:, None], above[3:6][:, None], positions, below[0:3][:, None], below[3:6][:, None]], axis=1
    )
    vertical = jnp.concatenate([above[6:7], stiff_v], axis=0)
    return wide, vertical


def surface_laplacian(extended):
    middle = extended[:, 1:-1]
    return (
        extended[:, 2:]
        + extended[:, :-2]
        + jnp.roll(middle, 1, axis=2)
        + jnp.roll(middle, -1, axis=2)
        - 4.0 * middle
    )


def membrane_force(positions, stiff_h, stiff_v):
    wide, vertical = halo(positions, stiff_v)
    middle = positions
    pulling = (
        stiff_h * (jnp.roll(middle, -1, axis=2) - middle)
        + jnp.roll(stiff_h, 1, axis=1) * (jnp.roll(middle, 1, axis=2) - middle)
        + vertical[1:] * (wide[:, 3:-1] - middle)
        + vertical[:-1] * (wide[:, 1:-3] - middle)
    )
    return pulling - bend_modulus * surface_laplacian(surface_laplacian(wide))


def one_hot(count, centred):
    shape = (count, centred.shape[1])
    row = (sublane(shape) - count // 2).astype(jnp.bfloat16)
    return jnp.where(row == centred, jnp.bfloat16(1), jnp.bfloat16(0))


def pack_kernel(owner_ref, element_ref, coords_ref, force_ref, out_ref, rank_ref, base_ref, acc_ref):
    owners, _, capacity = out_ref.shape
    markers = owner_ref.shape[1]
    row = lax.broadcasted_iota(jnp.int32, (LANES, LANES), 0)
    col = lax.broadcasted_iota(jnp.int32, (LANES, LANES), 1)
    before = jnp.where(row < col, 1.0, 0.0).astype(jnp.bfloat16)
    base_ref[...] = jnp.zeros_like(base_ref)
    acc_ref[...] = jnp.zeros_like(acc_ref)

    def ranks(r, carry):
        at = pl.ds(pl.multiple_of(r * LANES, LANES), LANES)
        own = owner_ref[:, at]
        hot = jnp.where(sublane((owners, LANES)) == own, 1.0, 0.0)
        earlier = dot(hot.astype(jnp.bfloat16), before, NN) + base_ref[...]
        rank_ref[:, at] = jnp.sum(hot * earlier, axis=0, keepdims=True).astype(jnp.int32)
        base_ref[...] = base_ref[...] + jnp.sum(hot, axis=1, keepdims=True)
        return carry

    lax.fori_loop(0, markers // LANES, ranks, 0, unroll=8)
    rows = force_ref.shape[2]
    step = 2 * rows

    def route(r, carry):
        at = pl.ds(pl.multiple_of(r * step, step), step)
        own = jnp.broadcast_to(owner_ref[:, at].astype(jnp.float32), (16, step)).astype(jnp.bfloat16)
        rank = (rank_ref[:, at] - capacity // 2).astype(jnp.float32).astype(jnp.bfloat16)
        force = [
            jnp.concatenate([force_ref[k, pl.ds(2 * r, 1), :], force_ref[k, pl.ds(2 * r + 1, 1), :]], axis=1)
            for k in range(3)
        ]
        payload = jnp.concatenate(
            [
                coords_ref[:, at],
                *force,
                element_ref[:, at].astype(jnp.float32) + 1.0,
                jnp.zeros((1, step), jnp.float32),
            ],
            axis=0,
        )
        both = jnp.concatenate(split(payload), axis=0).astype(jnp.bfloat16)
        left = jnp.concatenate(
            [jnp.where(own == jnp.bfloat16(d), both, jnp.bfloat16(0)) for d in range(owners)], axis=0
        )
        acc_ref[...] += dot(left, one_hot(capacity, rank), NT)
        return carry

    lax.fori_loop(0, markers // step, route, 0)
    for d in range(owners):
        out_ref[d] = acc_ref[16 * d : 16 * d + 8] + acc_ref[16 * d + 8 : 16 * d + 16]


def place_kernel(got_ref, place_ref, range_ref, hot_ref):
    sources, _, capacity = got_ref.shape
    groups = range_ref.shape[0]
    row = lax.broadcasted_iota(jnp.int32, (capacity, capacity), 0)
    col = lax.broadcasted_iota(jnp.int32, (capacity, capacity), 1)
    before = jnp.where(row < col, 1.0, 0.0).astype(jnp.bfloat16)
    kind = sublane((groups, capacity)).astype(jnp.float32)
    for s in range(sources):
        group = jnp.floor((got_ref[s, 6:7, :] - 1.0) * (1.0 / GROUP))
        hot_ref[s * groups : (s + 1) * groups, :] = jnp.where(kind == group, 1.0, 0.0)
    earlier = dot(hot_ref[...].astype(jnp.bfloat16), before, NN)
    count = jnp.sum(hot_ref[...], axis=1, keepdims=True)
    total = jnp.zeros((groups, 1), jnp.float32)
    for s in range(sources):
        total = total + count[s * groups : (s + 1) * groups]
    start = jnp.zeros((groups, 1), jnp.float32)
    for g in range(groups):
        start = start + jnp.where(sublane((groups, 1)) > g, total[g : g + 1], 0.0)
    base = start + 1.0
    for s in range(sources):
        rows = slice(s * groups, (s + 1) * groups)
        spot = jnp.sum(hot_ref[rows, :] * (earlier[rows] + base), axis=0, keepdims=True) - 1.0
        place_ref[s : s + 1, :] = spot
        base = base + count[rows]
    edge = (lax.broadcasted_iota(jnp.int32, range_ref.shape, 1) * LANES).astype(jnp.float32)
    first = jnp.sum(jnp.where(start + total <= edge, 1.0, 0.0), axis=0, keepdims=True)
    first = jnp.minimum(first, groups - 1.0)
    last = jnp.sum(jnp.where(start < edge + LANES, 1.0, 0.0), axis=0, keepdims=True)
    filled = jnp.sum(total, axis=0, keepdims=True)
    used = jnp.floor((filled + (LANES - 1)) * (1.0 / LANES)) + jnp.zeros_like(first)
    which = sublane(range_ref.shape)
    range_ref[...] = jnp.where(which == 0, first, jnp.where(which == 1, last, used)).astype(jnp.int32)


def spots(place_ref, i, per):
    spot = jnp.concatenate([place_ref[pl.ds(i * per + j, 1), :] for j in range(per)], axis=1)
    high = jnp.floor(spot * (1.0 / LANES))
    return high, (spot - high * LANES - LANES // 2).astype(jnp.bfloat16)


def sort_kernel(got_ref, place_ref, out_ref, acc_ref):
    sources, _, capacity = got_ref.shape
    chunks = out_ref.shape[0]
    per = 2
    acc_ref[...] = jnp.zeros_like(acc_ref)

    def gather(i, carry):
        payload = jnp.concatenate([got_ref[i * per + j] for j in range(per)], axis=1)
        both = jnp.concatenate(split(payload), axis=0).astype(jnp.bfloat16)
        high, low = spots(place_ref, i, per)
        high = jnp.broadcast_to(high, (16, per * capacity)).astype(jnp.bfloat16)
        left = jnp.concatenate(
            [jnp.where(high == jnp.bfloat16(h), both, jnp.bfloat16(0)) for h in range(chunks)], axis=0
        )
        acc_ref[...] += dot(left, one_hot(LANES, low), NT)
        return carry

    lax.fori_loop(0, sources // per, gather, 0)
    for h in range(chunks):
        out_ref[h] = acc_ref[16 * h : 16 * h + 8] + acc_ref[16 * h + 8 : 16 * h + 16]


def return_kernel(place_ref, sampled_ref, out_ref):
    sources, _, capacity = out_ref.shape
    chunks = sampled_ref.shape[0]
    per = 2
    rows = []
    for h in range(chunks):
        rows.extend(split(sampled_ref[h]))
    table = jnp.concatenate(rows, axis=0).astype(jnp.bfloat16)

    def scatter(i, carry):
        high, low = spots(place_ref, i, per)
        high = jnp.broadcast_to(high, (8, per * capacity))
        picked = dot(table, one_hot(LANES, low), NN)
        total = jnp.zeros((8, per * capacity), jnp.float32)
        for h in range(chunks):
            total = total + jnp.where(high == float(h), picked[8 * h : 8 * h + 8], 0.0)
        total = total[0:4] + total[4:8]
        for j in range(per):
            out_ref[i * per + j] = total[:, j * capacity : (j + 1) * capacity]
        return carry

    lax.fori_loop(0, sources // per, scatter, 0)


def basis_rows(x):
    node = sublane((POINTS, x.shape[1]))
    value = jnp.zeros((POINTS, x.shape[1]), jnp.float32)
    for i in range(POINTS):
        value = jnp.where(node == i, float(SCALE[i]), value)
    for j in range(POINTS):
        value = value * jnp.where(node == j, 1.0, x - float(ABSCISSA[j]))
    return value


def build_weights(payload, weight_ref):
    along_r = basis_rows(payload[0:1])
    along_s = basis_rows(payload[1:2])
    along_t = basis_rows(payload[2:3])
    plane = jnp.concatenate([along_s[b : b + 1] * along_t for b in range(POINTS)], axis=0)
    step = POINTS * POINTS
    for a in range(POINTS):
        block = along_r[a : a + 1] * plane
        high = block.astype(jnp.bfloat16)
        weight_ref[0, a * step : (a + 1) * step, :] = high
        weight_ref[1, a * step : (a + 1) * step, :] = (block - high.astype(jnp.float32)).astype(jnp.bfloat16)


def prepare_kernel(velocity_ref, out_ref):
    groups = out_ref.shape[0]
    for g in range(groups):
        for k in range(3):
            high, low = split(velocity_ref[k, g * GROUP : (g + 1) * GROUP, :])
            out_ref[g, k * GROUP : (k + 1) * GROUP, :] = high.astype(jnp.bfloat16)
            out_ref[g, (3 + k) * GROUP : (4 + k) * GROUP, :] = low.astype(jnp.bfloat16)


def hot_elements(payload, g):
    return jnp.where(
        sublane((GROUP, LANES)).astype(jnp.float32) + (g * GROUP + 1).astype(jnp.float32) == payload[6:7], 1.0, 0.0
    )


def sample_kernel(range_ref, sorted_ref, velocity_ref, out_ref, even_ref, odd_ref):
    used = range_ref[2, 0]
    out_ref[...] = jnp.zeros_like(out_ref)

    def visit(c, g, weight_ref):
        wide = dot(velocity_ref[g], weight_ref[0], NN)
        narrow = dot(velocity_ref[g, 0 : 3 * GROUP], weight_ref[1], NN)
        total = wide[: 3 * GROUP] + wide[3 * GROUP :] + narrow
        hot = hot_elements(sorted_ref[c], g)
        sums = [jnp.sum(hot * total[k * GROUP : (k + 1) * GROUP], axis=0, keepdims=True) for k in range(3)]
        out_ref[c] += jnp.concatenate(sums + [jnp.zeros((1, LANES), jnp.float32)], axis=0)

    pipeline(range_ref, used, visit, sorted_ref, even_ref, odd_ref)


def pipeline(range_ref, used, visit, sorted_ref, even_ref, odd_ref):
    last = sorted_ref.shape[0] - 1
    build_weights(sorted_ref[0], even_ref)

    def half(c, this_ref, next_ref):
        visit(c, range_ref[0, c], this_ref)
        build_weights(sorted_ref[jnp.minimum(c + 1, last)], next_ref)

        def more(g, carry):
            visit(c, g, this_ref)
            return carry

        lax.fori_loop(range_ref[0, c] + 1, range_ref[1, c], more, 0)

    def pair(i, carry):
        half(2 * i, even_ref, odd_ref)
        half(2 * i + 1, odd_ref, even_ref)
        return carry

    lax.fori_loop(0, (used + 1) // 2, pair, 0)


def deposit_kernel(range_ref, sorted_ref, out_ref, even_ref, odd_ref):
    used = range_ref[2, 0]
    out_ref[...] = jnp.zeros_like(out_ref)

    def visit(c, g, weight_ref):
        payload = sorted_ref[c]
        hot = hot_elements(payload, g)
        high, low = split(payload)
        left = jnp.concatenate(
            [hot * part[3 + k : 4 + k] for part in (high, low) for k in range(3)], axis=0
        ).astype(jnp.bfloat16)
        wide = dot(left, weight_ref[0], NT)
        narrow = dot(left[: 3 * GROUP], weight_ref[1], NT)
        total = wide[: 3 * GROUP] + wide[3 * GROUP :] + narrow
        rows = pl.ds(pl.multiple_of(g * GROUP, GROUP), GROUP)
        for k in range(3):
            out_ref[k, rows, :] += total[k * GROUP : (k + 1) * GROUP]

    pipeline(range_ref, used, visit, sorted_ref, even_ref, odd_ref)


def unpack_kernel(owner_ref, rank_ref, arrived_ref, positions_ref, out_ref):
    owners, _, capacity = arrived_ref.shape
    chunks = owner_ref.shape[1] // LANES
    rows = []
    for d in range(owners):
        rows.extend(split(arrived_ref[d]))
    table = jnp.concatenate(rows, axis=0).astype(jnp.bfloat16)

    def chunk(r, carry):
        at = pl.ds(pl.multiple_of(r * LANES, LANES), LANES)
        own = jnp.broadcast_to(owner_ref[:, at], (8, LANES))
        rank = (rank_ref[:, at] - capacity // 2).astype(jnp.float32).astype(jnp.bfloat16)
        picked = dot(table, one_hot(capacity, rank), NN)
        total = jnp.zeros((8, LANES), jnp.float32)
        for d in range(owners):
            total = total + jnp.where(own == d, picked[8 * d : 8 * d + 8], 0.0)
        for k in range(3):
            moved = total[k : k + 1] + total[4 + k : 5 + k]
            out_ref[k, pl.ds(r, 1), :] = positions_ref[k, pl.ds(r, 1), :] + time_step * moved
        return carry

    lax.fori_loop(0, chunks, chunk, 0, unroll=2)


def exchange(x):
    return lax.all_to_all(x, AXES, 0, 0, tiled=True)


def local(velocity, positions, stiff_h, stiff_v, marker_owner, marker_element, marker_coords):
    devices = lax.axis_size(AXES)
    markers = marker_owner.shape[0]
    capacity = 3 * markers // (2 * devices)
    slots = devices * capacity
    elements = velocity.shape[1]
    groups = elements // GROUP
    f32 = jnp.float32

    force = membrane_force(positions, stiff_h, stiff_v)
    owner = marker_owner.reshape(1, markers)
    element = marker_element.reshape(1, markers)
    outgoing, rank = pl.pallas_call(
        pack_kernel,
        out_shape=(
            jax.ShapeDtypeStruct((devices, 8, capacity), f32),
            jax.ShapeDtypeStruct((1, markers), jnp.int32),
        ),
        scratch_shapes=[pltpu.VMEM((devices, 1), f32), pltpu.VMEM((devices * 16, capacity), f32)],
        name="pack",
    )(owner, element, marker_coords, force)
    got = exchange(outgoing)
    table = pl.pallas_call(
        prepare_kernel,
        out_shape=jax.ShapeDtypeStruct((groups, 6 * GROUP, NODES), jnp.bfloat16),
        name="prepare",
    )(velocity)
    chunks = slots // LANES
    place, spans = pl.pallas_call(
        place_kernel,
        out_shape=(
            jax.ShapeDtypeStruct((devices, capacity), f32),
            jax.ShapeDtypeStruct((groups, 128), jnp.int32),
        ),
        scratch_shapes=[pltpu.VMEM((devices * groups, capacity), f32)],
        name="place",
    )(got)
    ordered = pl.pallas_call(
        sort_kernel,
        out_shape=jax.ShapeDtypeStruct((chunks, 8, LANES), f32),
        scratch_shapes=[pltpu.VMEM((chunks * 16, LANES), f32)],
        name="sort",
    )(got, place)
    weights = pltpu.VMEM((2, NODES, LANES), jnp.bfloat16)
    scalars = pl.BlockSpec(memory_space=pltpu.SMEM)
    vector = pl.BlockSpec(memory_space=pltpu.VMEM)
    sampled = pl.pallas_call(
        sample_kernel,
        out_shape=jax.ShapeDtypeStruct((chunks, 4, LANES), f32),
        in_specs=[scalars, vector, vector],
        scratch_shapes=[weights, weights],
        name="sample",
    )(spans, ordered, table)
    returning = pl.pallas_call(
        return_kernel,
        out_shape=jax.ShapeDtypeStruct((devices, 4, capacity), f32),
        name="return",
    )(place, sampled)
    arrived = exchange(returning)
    node_forces = pl.pallas_call(
        deposit_kernel,
        out_shape=jax.ShapeDtypeStruct(velocity.shape, f32),
        in_specs=[scalars, vector],
        scratch_shapes=[weights, weights],
        name="deposit",
    )(spans, ordered)
    moved = pl.pallas_call(
        unpack_kernel,
        out_shape=jax.ShapeDtypeStruct(positions.shape, f32),
        name="unpack",
    )(owner, rank, arrived, positions)
    return moved, node_forces


def solution(mesh):
    return jax.shard_map(
        local,
        mesh=mesh,
        in_specs=(
            P(None, AXES, None),
            P(None, AXES, None),
            P(AXES, None),
            P(AXES, None),
            P(AXES, None),
            P(AXES),
            P(None, AXES),
        ),
        out_specs=(P(None, AXES, None), P(None, AXES, None)),
        check_vma=False,
    )
```

```python
import functools

import jax
import jax.numpy as jnp
import numpy as np
from jax import lax
from jax.experimental import pallas as pl
from jax.experimental.pallas import tpu as pltpu
from jax.sharding import PartitionSpec as P

POINTS = 8
NODES = POINTS * POINTS * POINTS
AXES = ("gx", "gy")
SMALL = pltpu.CompilerParams(vmem_limit_bytes=20 * 1024 * 1024)
LANES = 256
GROUP = 32
DEPTH = 4

bend_modulus = 0.05
time_step = 0.5

ABSCISSA = -np.cos(np.pi * np.arange(POINTS) / (POINTS - 1))
SCALE = np.array(
    [1.0 / np.prod([ABSCISSA[i] - ABSCISSA[j] for j in range(POINTS) if j != i]) for i in range(POINTS)]
)

NN = (((1,), (0,)), ((), ()))
NT = (((1,), (1,)), ((), ()))


def dot(a, b, dims):
    return lax.dot_general(a, b, dims, preferred_element_type=jnp.float32)


def split(x):
    high = x.astype(jnp.bfloat16).astype(jnp.float32)
    return high, x - high


def sublane(shape):
    return lax.broadcasted_iota(jnp.int32, shape, 0)


def halo(positions, stiff_v):
    count = lax.axis_size(AXES)
    tail = jnp.concatenate([positions[:, -2], positions[:, -1], stiff_v[-1:]], axis=0)
    head = jnp.concatenate([positions[:, 0], positions[:, 1]], axis=0)
    above = lax.ppermute(tail, AXES, [(i, (i + 1) % count) for i in range(count)])
    below = lax.ppermute(head, AXES, [((i + 1) % count, i) for i in range(count)])
    return above, below


def around(x, rows, cols):
    if rows:
        return pltpu.roll(x, rows % x.shape[0], 0)
    return pltpu.roll(x, cols % x.shape[1], 1)


def surface_laplacian(x):
    return around(x, -1, 0) + around(x, 1, 0) + around(x, 0, 1) + around(x, 0, -1) - 4.0 * x


def membrane_force(positions_ref, above_ref, below_ref, stiff_h_ref, stiff_v_ref, wide_ref, force_ref):
    rows = stiff_h_ref.shape[0]
    inner = slice(8, 8 + rows)
    stiff_h = stiff_h_ref[...]
    stiff_v = stiff_v_ref[...]
    wide_ref[3, inner, :] = stiff_v
    wide_ref[3, 7:8, :] = above_ref[6:7]
    stiff_before = wide_ref[3, 7 : 7 + rows, :]
    for k in range(3):
        wide_ref[k, inner, :] = positions_ref[k]
        wide_ref[k, 6:7, :] = above_ref[k : k + 1]
        wide_ref[k, 7:8, :] = above_ref[3 + k : 4 + k]
        wide_ref[k, 8 + rows : 9 + rows, :] = below_ref[k : k + 1]
        wide_ref[k, 9 + rows : 10 + rows, :] = below_ref[3 + k : 4 + k]
        wide = wide_ref[k]
        middle = wide[inner]
        pulling = (
            stiff_h * (around(middle, 0, -1) - middle)
            + around(stiff_h, 0, 1) * (around(middle, 0, 1) - middle)
            + stiff_v * (around(wide, -1, 0)[inner] - middle)
            + stiff_before * (around(wide, 1, 0)[inner] - middle)
        )
        bending = surface_laplacian(surface_laplacian(wide))[inner]
        force_ref[k] = pulling - bend_modulus * bending


def one_hot(count, centred):
    shape = (count, centred.shape[1])
    row = (sublane(shape) - count // 2).astype(jnp.bfloat16)
    return jnp.where(row == centred, jnp.bfloat16(1), jnp.bfloat16(0))


def fetch(pairs, sems):
    copies = [pltpu.make_async_copy(far, here, sems.at[i]) for i, (far, here) in enumerate(pairs)]
    for copy in copies:
        copy.start()
    for copy in copies:
        copy.wait()


def rank_kernel(owner_far, rank_ref, owner_ref, base_ref, sems):
    fetch([(owner_far, owner_ref)], sems)
    owners = base_ref.shape[0]
    row = lax.broadcasted_iota(jnp.int32, (LANES, LANES), 0)
    col = lax.broadcasted_iota(jnp.int32, (LANES, LANES), 1)
    before = jnp.where(row < col, 1.0, 0.0).astype(jnp.bfloat16)
    base_ref[...] = jnp.zeros_like(base_ref)

    def ranks(r, carry):
        at = pl.ds(pl.multiple_of(r * LANES, LANES), LANES)
        own = owner_ref[:, at]
        hot = jnp.where(sublane((owners, LANES)) == own, 1.0, 0.0)
        earlier = dot(hot.astype(jnp.bfloat16), before, NN) + base_ref[...]
        rank_ref[:, at] = jnp.sum(hot * earlier, axis=0, keepdims=True)
        base_ref[...] = base_ref[...] + jnp.sum(hot, axis=1, keepdims=True)
        return carry

    lax.fori_loop(0, owner_ref.shape[1] // LANES, ranks, 0, unroll=8)


def pack_kernel(
    rank_far,
    owner_far,
    element_far,
    coords_far,
    positions_far,
    stiff_h_far,
    stiff_v_far,
    above_ref,
    below_ref,
    out_ref,
    rank_ref,
    owner_ref,
    element_ref,
    coords_ref,
    positions_ref,
    stiff_h_ref,
    stiff_v_ref,
    wide_ref,
    force_ref,
    acc_ref,
    sems,
    *,
    capacity,
):
    fetch(
        [
            (rank_far, rank_ref),
            (owner_far, owner_ref),
            (element_far, element_ref),
            (coords_far, coords_ref),
            (positions_far, positions_ref),
            (stiff_h_far, stiff_h_ref),
            (stiff_v_far, stiff_v_ref),
        ],
        sems,
    )
    units, _, unit = out_ref.shape
    width = acc_ref.shape[1]
    blocks = units * unit // width
    markers = owner_ref.shape[1]
    columns = force_ref.shape[2]
    lines = 4
    step = lines * columns
    membrane_force(positions_ref, above_ref, below_ref, stiff_h_ref, stiff_v_ref, wide_ref, force_ref)
    acc_ref[...] = jnp.zeros_like(acc_ref)

    def route(r, carry):
        at = pl.ds(pl.multiple_of(r * step, step), step)
        slot = owner_ref[:, at].astype(jnp.float32) * float(capacity) + rank_ref[:, at]
        block = jnp.floor((slot + 0.5) * (1.0 / width))
        inside = (slot - block * width - width // 2).astype(jnp.bfloat16)
        block = jnp.broadcast_to(block, (16, step)).astype(jnp.bfloat16)
        force = [
            jnp.concatenate([force_ref[k, pl.ds(lines * r + i, 1), :] for i in range(lines)], axis=1)
            for k in range(3)
        ]
        payload = jnp.concatenate(
            [
                coords_ref[:, at],
                *force,
                element_ref[:, at].astype(jnp.float32) + 1.0,
                jnp.zeros((1, step), jnp.float32),
            ],
            axis=0,
        )
        both = jnp.concatenate(split(payload), axis=0).astype(jnp.bfloat16)
        left = jnp.concatenate(
            [jnp.where(block == jnp.bfloat16(h), both, jnp.bfloat16(0)) for h in range(blocks)], axis=0
        )
        acc_ref[...] += dot(left, one_hot(width, inside), NT)
        return carry

    lax.fori_loop(0, markers // step, route, 0)
    for u in range(units):
        h, at = u * unit // width, u * unit % width
        out_ref[u] = acc_ref[16 * h : 16 * h + 8, at : at + unit] + acc_ref[16 * h + 8 : 16 * h + 16, at : at + unit]


def block_of(got_ref, i, per, capacity):
    count = per * capacity // got_ref.shape[2]
    return jnp.concatenate([got_ref[i * count + j] for j in range(count)], axis=1)


def find_places(got_ref, place_ref, range_ref, hot_ref):
    sources, capacity = place_ref.shape
    groups = range_ref.shape[0]
    row = lax.broadcasted_iota(jnp.int32, (capacity, capacity), 0)
    col = lax.broadcasted_iota(jnp.int32, (capacity, capacity), 1)
    before = jnp.where(row < col, 1.0, 0.0).astype(jnp.bfloat16)
    kind = sublane((groups, capacity)).astype(jnp.float32)
    for s in range(sources):
        group = jnp.floor((block_of(got_ref, s, 1, capacity)[6:7] - 1.0) * (1.0 / GROUP))
        hot_ref[s * groups : (s + 1) * groups, :] = jnp.where(kind == group, 1.0, 0.0)
    earlier = dot(hot_ref[...].astype(jnp.bfloat16), before, NN)
    count = jnp.sum(hot_ref[...], axis=1, keepdims=True)
    total = jnp.zeros((groups, 1), jnp.float32)
    for s in range(sources):
        total = total + count[s * groups : (s + 1) * groups]
    total = jnp.floor((total + (LANES - 1)) * (1.0 / LANES)) * LANES
    start = jnp.zeros((groups, 1), jnp.float32)
    for g in range(groups):
        start = start + jnp.where(sublane((groups, 1)) > g, total[g : g + 1], 0.0)
    base = start + 1.0
    for s in range(sources):
        rows = slice(s * groups, (s + 1) * groups)
        spot = jnp.sum(hot_ref[rows, :] * (earlier[rows] + base), axis=0, keepdims=True) - 1.0
        place_ref[s : s + 1, :] = spot
        base = base + count[rows]
    edge = (lax.broadcasted_iota(jnp.int32, range_ref.shape, 1) * LANES).astype(jnp.float32)
    group = jnp.sum(jnp.where(start + total <= edge, 1.0, 0.0), axis=0, keepdims=True)
    group = jnp.minimum(group, groups - 1.0)
    used = jnp.sum(total, axis=0, keepdims=True) * (1.0 / LANES) + jnp.zeros_like(group)
    range_ref[...] = jnp.where(sublane(range_ref.shape) == 0, group, used).astype(jnp.int32)


def spots(place_ref, i, per):
    spot = jnp.concatenate([place_ref[pl.ds(i * per + j, 1), :] for j in range(per)], axis=1)
    high = jnp.floor(spot * (1.0 / LANES))
    return high, (spot - high * LANES - LANES // 2).astype(jnp.bfloat16)


def batch_of(sources, capacity):
    per = 1
    while per < sources and (per * capacity) % 512 != 0:
        per *= 2
    return per


def sort_markers(got_ref, place_ref, out_ref, acc_ref):
    sources, capacity = place_ref.shape
    chunks = out_ref.shape[0]
    per = batch_of(sources, capacity)
    acc_ref[...] = jnp.zeros_like(acc_ref)

    def gather(i, carry):
        payload = block_of(got_ref, i, per, capacity)
        both = jnp.concatenate(split(payload), axis=0).astype(jnp.bfloat16)
        high, low = spots(place_ref, i, per)
        high = jnp.broadcast_to(high, (16, per * capacity)).astype(jnp.bfloat16)
        left = jnp.concatenate(
            [jnp.where(high == jnp.bfloat16(h), both, jnp.bfloat16(0)) for h in range(chunks)], axis=0
        )
        acc_ref[...] += dot(left, one_hot(LANES, low), NT)
        return carry

    lax.fori_loop(0, sources // per, gather, 0)
    for h in range(chunks):
        out_ref[h] = acc_ref[16 * h : 16 * h + 8] + acc_ref[16 * h + 8 : 16 * h + 16]


def return_samples(place_ref, sampled_ref, out_ref):
    sources, _, capacity = out_ref.shape
    chunks = sampled_ref.shape[0] // 8
    per = batch_of(sources, capacity)
    table = sampled_ref[...].astype(jnp.bfloat16)

    def scatter(i, carry):
        high, low = spots(place_ref, i, per)
        high = jnp.broadcast_to(high, (8, per * capacity))
        picked = dot(table, one_hot(LANES, low), NN)
        total = jnp.zeros((8, per * capacity), jnp.float32)
        for h in range(chunks):
            total = jnp.where(high == float(h), picked[8 * h : 8 * h + 8], total)
        total = total[0:4] + total[4:8]
        for j in range(per):
            out_ref[i * per + j] = total[:, j * capacity : (j + 1) * capacity]
        return carry

    lax.fori_loop(0, sources // per, scatter, 0)


def basis_rows(x):
    node = sublane((POINTS, x.shape[1]))
    value = jnp.zeros((POINTS, x.shape[1]), jnp.float32)
    for i in range(POINTS):
        value = jnp.where(node == i, float(SCALE[i]), value)
    for j in range(POINTS):
        value = value * jnp.where(node == j, 1.0, x - float(ABSCISSA[j]))
    return value


def build_weights(payload, weight_ref):
    along_r = basis_rows(payload[0:1])
    along_s = basis_rows(payload[1:2])
    along_t = basis_rows(payload[2:3])
    step = POINTS * POINTS
    for lane in range(0, LANES, 128):
        at = slice(lane, lane + 128)
        t = along_t[:, at]
        plane = jnp.concatenate([along_s[b : b + 1, at] * t for b in range(POINTS)], axis=0)
        for a in range(POINTS):
            block = along_r[a : a + 1, at] * plane
            high = block.astype(jnp.bfloat16)
            weight_ref[0, a * step : (a + 1) * step, at] = high
            weight_ref[1, a * step : (a + 1) * step, at] = (block - high.astype(jnp.float32)).astype(jnp.bfloat16)


def prepare_kernel(velocity_ref, out_ref):
    groups = out_ref.shape[0]
    for g in range(groups):
        for k in range(3):
            high, low = split(velocity_ref[k, g * GROUP : (g + 1) * GROUP, :])
            out_ref[g, k * GROUP : (k + 1) * GROUP, :] = high.astype(jnp.bfloat16)
            out_ref[g, (3 + k) * GROUP : (4 + k) * GROUP, :] = low.astype(jnp.bfloat16)


def hot_elements(payload, g):
    return jnp.where(
        sublane((GROUP, LANES)).astype(jnp.float32) + (g * GROUP + 1).astype(jnp.float32) == payload[6:7], 1.0, 0.0
    )


def pipeline(range_ref, visit, sorted_ref, weight_refs):
    depth = len(weight_refs)
    last = sorted_ref.shape[0] - 1
    for j in range(depth):
        build_weights(sorted_ref[j], weight_refs[j])

    def several(i, carry):
        for j in range(depth):
            c = depth * i + j
            visit(c, range_ref[0, c], weight_refs[j])
            build_weights(sorted_ref[jnp.minimum(c + depth, last)], weight_refs[j])
        return carry

    lax.fori_loop(0, (range_ref[1, 0] + (depth - 1)) // depth, several, 0)


def interpolate_kernel(
    got_ref,
    velocity_ref,
    out_ref,
    sorted_ref,
    range_ref,
    place_ref,
    hot_ref,
    acc_ref,
    sampled_ref,
    scalar_ref,
    sem_ref,
    *weight_refs,
):
    find_places(got_ref, place_ref, range_ref, hot_ref)
    spans = pltpu.make_async_copy(range_ref, scalar_ref, sem_ref)
    spans.start()
    sort_markers(got_ref, place_ref, sorted_ref, acc_ref)
    spans.wait()
    sampled_ref[...] = jnp.zeros_like(sampled_ref)

    def visit(c, g, weight_ref):
        wide = dot(velocity_ref[g], weight_ref[0], NN)
        narrow = dot(velocity_ref[g, 0 : 3 * GROUP], weight_ref[1], NN)
        total = wide[: 3 * GROUP] + wide[3 * GROUP :] + narrow
        hot = hot_elements(sorted_ref[c], g)
        sums = [jnp.sum(hot * total[k * GROUP : (k + 1) * GROUP], axis=0, keepdims=True) for k in range(3)]
        parts = split(jnp.concatenate(sums + [jnp.zeros((1, LANES), jnp.float32)], axis=0))
        sampled_ref[pl.ds(pl.multiple_of(c * 8, 8), 8), :] = jnp.concatenate(parts, axis=0)

    pipeline(scalar_ref, visit, sorted_ref, weight_refs)
    return_samples(place_ref, sampled_ref, out_ref)


def deposit_kernel(range_ref, sorted_ref, out_ref, *weight_refs):
    out_ref[...] = jnp.zeros_like(out_ref)

    def visit(c, g, weight_ref):
        payload = sorted_ref[c]
        hot = hot_elements(payload, g)
        left = jnp.concatenate(
            [hot * part[3 + k : 4 + k] for part in split(payload) for k in range(3)], axis=0
        ).astype(jnp.bfloat16)
        wide = dot(left, weight_ref[0], NT)
        narrow = dot(left[: 3 * GROUP], weight_ref[1], NT)
        total = wide[: 3 * GROUP] + wide[3 * GROUP :] + narrow
        rows = pl.ds(pl.multiple_of(g * GROUP, GROUP), GROUP)
        for k in range(3):
            out_ref[k, rows, :] += total[k * GROUP : (k + 1) * GROUP]

    pipeline(range_ref, visit, sorted_ref, weight_refs)


def unpack_kernel(owner_ref, rank_ref, arrived_ref, positions_ref, out_ref):
    owners, _, capacity = arrived_ref.shape
    columns = positions_ref.shape[2]
    lines = 4
    step = lines * columns
    rows = []
    for d in range(owners):
        rows.extend(split(arrived_ref[d]))
    table = jnp.concatenate(rows, axis=0).astype(jnp.bfloat16)

    def chunk(r, carry):
        at = pl.ds(pl.multiple_of(r * step, step), step)
        own = jnp.broadcast_to(owner_ref[:, at], (8, step))
        rank = (rank_ref[:, at] - capacity // 2).astype(jnp.bfloat16)
        picked = dot(table, one_hot(capacity, rank), NN)
        total = jnp.zeros((8, step), jnp.float32)
        for d in range(owners):
            total = jnp.where(own == d, picked[8 * d : 8 * d + 8], total)
        moved = total[0:4] + total[4:8]
        for k in range(3):
            for i in range(lines):
                row = pl.ds(lines * r + i, 1)
                part = moved[k : k + 1, i * columns : (i + 1) * columns]
                out_ref[k, row, :] = positions_ref[k, row, :] + time_step * part
        return carry

    lax.fori_loop(0, owner_ref.shape[1] // step, chunk, 0)


def near(*arrays):
    return [pltpu.with_memory_space_constraint(x, pltpu.VMEM) for x in arrays]


def away(*arrays):
    return [pltpu.with_memory_space_constraint(x, pltpu.HBM) for x in arrays]


def exchange(x):
    return lax.all_to_all(x, AXES, 0, 0, tiled=True)


def local(velocity, positions, stiff_h, stiff_v, marker_owner, marker_element, marker_coords):
    devices = lax.axis_size(AXES)
    markers = marker_owner.shape[0]
    capacity = 3 * markers // (2 * devices)
    slots = devices * capacity
    elements = velocity.shape[1]
    groups = elements // GROUP
    f32 = jnp.float32

    above, below = halo(positions, stiff_v)
    owner = marker_owner.reshape(1, markers)
    element = marker_element.reshape(1, markers)
    hbm = pl.BlockSpec(memory_space=pltpu.HBM)
    vector = pl.BlockSpec(memory_space=pltpu.VMEM)
    rank = pl.pallas_call(
        rank_kernel,
        out_shape=jax.ShapeDtypeStruct((1, markers), f32),
        in_specs=[hbm],
        scratch_shapes=[
            pltpu.VMEM((1, markers), jnp.int32),
            pltpu.VMEM((devices, 1), f32),
            pltpu.SemaphoreType.DMA((1,)),
        ],
        compiler_params=SMALL,
        name="rank",
    )(*away(owner))
    rows, columns = stiff_h.shape
    whole = capacity % 128 == 0 and slots % LANES == 0
    unit = 128 if whole else capacity
    width = LANES if whole else capacity
    far = (rank, owner, element, marker_coords, positions, stiff_h, stiff_v)
    outgoing = pl.pallas_call(
        functools.partial(pack_kernel, capacity=capacity),
        out_shape=jax.ShapeDtypeStruct((slots // unit, 8, unit), f32),
        in_specs=[hbm] * 7 + [vector] * 2,
        scratch_shapes=[
            *[pltpu.VMEM(x.shape, x.dtype) for x in far],
            pltpu.VMEM((4, rows + 16, columns), f32),
            pltpu.VMEM((3, rows, columns), f32),
            pltpu.VMEM((slots // width * 16, width), f32),
            pltpu.SemaphoreType.DMA((7,)),
        ],
        compiler_params=SMALL,
        name="pack",
    )(*away(*far), *near(above, below))
    got = exchange(outgoing)
    table = pl.pallas_call(
        prepare_kernel,
        out_shape=pltpu.VMEM((groups, 6 * GROUP, NODES), jnp.bfloat16),
        compiler_params=SMALL,
        name="prepare",
    )(*near(velocity))
    chunks = slots // LANES + groups
    weights = pltpu.VMEM((2, NODES, LANES), jnp.bfloat16)
    returning, ordered, spans = pl.pallas_call(
        interpolate_kernel,
        out_shape=(
            pltpu.VMEM((devices, 4, capacity), f32),
            pltpu.VMEM((chunks, 8, LANES), f32),
            jax.ShapeDtypeStruct((groups, 128), jnp.int32),
        ),
        scratch_shapes=[
            pltpu.VMEM((devices, capacity), f32),
            pltpu.VMEM((devices * groups, capacity), f32),
            pltpu.VMEM((chunks * 16, LANES), f32),
            pltpu.VMEM((chunks * 8, LANES), f32),
            pltpu.SMEM((groups, 128), jnp.int32),
            pltpu.SemaphoreType.DMA,
            *[weights] * DEPTH,
        ],
        compiler_params=SMALL,
        name="interpolate",
    )(*near(got, table))
    arrived = exchange(returning)
    node_forces = pl.pallas_call(
        deposit_kernel,
        out_shape=jax.ShapeDtypeStruct(velocity.shape, f32),
        in_specs=[pl.BlockSpec(memory_space=pltpu.SMEM), pl.BlockSpec(memory_space=pltpu.VMEM)],
        scratch_shapes=[weights] * DEPTH,
        compiler_params=SMALL,
        name="deposit",
    )(spans, *near(ordered))
    moved = pl.pallas_call(
        unpack_kernel,
        out_shape=jax.ShapeDtypeStruct(positions.shape, f32),
        compiler_params=SMALL,
        name="unpack",
    )(*near(owner, rank, arrived, positions))
    return moved, node_forces


def solution(mesh):
    return jax.shard_map(
        local,
        mesh=mesh,
        in_specs=(
            P(None, AXES, None),
            P(None, AXES, None),
            P(AXES, None),
            P(AXES, None),
            P(AXES, None),
            P(AXES),
            P(None, AXES),
        ),
        out_specs=(P(None, AXES, None), P(None, AXES, None)),
        check_vma=False,
    )
```

```python
import functools

import jax
import jax.numpy as jnp
import numpy as np
from jax import lax
from jax.experimental import pallas as pl
from jax.experimental.pallas import tpu as pltpu
from jax.sharding import PartitionSpec as P

POINTS = 8
AXES = ("gx", "gy")
SMALL = pltpu.CompilerParams(vmem_limit_bytes=20 * 1024 * 1024)
LANES = 256
GROUP = 32
DEPTH = 4

bend_modulus = 0.05
time_step = 0.5

ABSCISSA = -np.cos(np.pi * np.arange(POINTS) / (POINTS - 1))
SCALE = np.array(
    [1.0 / np.prod([ABSCISSA[i] - ABSCISSA[j] for j in range(POINTS) if j != i]) for i in range(POINTS)]
)

NN = (((1,), (0,)), ((), ()))
NT = (((1,), (1,)), ((), ()))


def dot(a, b, dims):
    return lax.dot_general(a, b, dims, preferred_element_type=jnp.float32)


def split(x):
    high = x.astype(jnp.bfloat16).astype(jnp.float32)
    return high, x - high


def sublane(shape):
    return lax.broadcasted_iota(jnp.int32, shape, 0)


def halo(positions, stiff_v):
    count = lax.axis_size(AXES)
    stacked = jnp.concatenate([positions, stiff_v[None]], axis=0)
    tail = stacked[:, -2:]
    head = stacked[:, :2]
    above = lax.ppermute(tail, AXES, [(i, (i + 1) % count) for i in range(count)])
    below = lax.ppermute(head, AXES, [((i + 1) % count, i) for i in range(count)])
    return above, below


def around(x, rows, cols):
    if rows:
        return pltpu.roll(x, rows % x.shape[0], 0)
    return pltpu.roll(x, cols % x.shape[1], 1)


def surface_laplacian(x):
    return around(x, -1, 0) + around(x, 1, 0) + around(x, 0, 1) + around(x, 0, -1) - 4.0 * x


def membrane_force(positions_ref, above_ref, below_ref, stiff_h_ref, stiff_v_ref, wide_ref, force_ref):
    rows = stiff_h_ref.shape[0]
    inner = slice(8, 8 + rows)
    stiff_h = stiff_h_ref[...]
    stiff_v = stiff_v_ref[...]
    wide_ref[3, inner, :] = stiff_v
    wide_ref[3, 7:8, :] = above_ref[3, 1:2, :]
    stiff_before = wide_ref[3, 7 : 7 + rows, :]
    for k in range(3):
        wide_ref[k, inner, :] = positions_ref[k]
        wide_ref[k, 6:8, :] = above_ref[k]
        wide_ref[k, 8 + rows : 10 + rows, :] = below_ref[k]
        wide = wide_ref[k]
        middle = wide[inner]
        pulling = (
            stiff_h * (around(middle, 0, -1) - middle)
            + around(stiff_h, 0, 1) * (around(middle, 0, 1) - middle)
            + stiff_v * (around(wide, -1, 0)[inner] - middle)
            + stiff_before * (around(wide, 1, 0)[inner] - middle)
        )
        bending = surface_laplacian(surface_laplacian(wide))[inner]
        force_ref[k] = pulling - bend_modulus * bending


def one_hot(count, centred):
    shape = (count, centred.shape[1])
    row = (sublane(shape) - count // 2).astype(jnp.bfloat16)
    return jnp.where(row == centred, jnp.bfloat16(1), jnp.bfloat16(0))


def spread(payload, label, count):
    wide = jnp.broadcast_to(label, (16, label.shape[1]))
    wide = (wide - (sublane(wide.shape) // 8).astype(jnp.float32)).astype(jnp.bfloat16)
    masks = [wide == jnp.bfloat16(2 * i) for i in range(count // 2)]
    sides = []
    for part in split(payload):
        twice = jnp.concatenate([part, part], axis=0).astype(jnp.bfloat16)
        sides.append(jnp.concatenate([jnp.where(mask, twice, jnp.bfloat16(0)) for mask in masks], axis=0))
    return jnp.concatenate(sides, axis=0)


def fold(x):
    half = x.shape[0] // 2
    return x[:half] + x[half:]


def pick(rows, label, right):
    parts = [part.astype(jnp.bfloat16) for part in split(rows)]
    if rows.shape[1] % 128 == 0:
        found = dot(jnp.concatenate(parts, axis=1), jnp.concatenate([right, right], axis=0), NN)
    else:
        found = dot(parts[0], right, NN) + dot(parts[1], right, NN)
    wide = jnp.broadcast_to(label, (8, label.shape[1]))
    wide = wide - (sublane(wide.shape) // 4).astype(jnp.float32)
    total = jnp.zeros(wide.shape, jnp.float32)
    for i in range(rows.shape[0] // 8):
        total = jnp.where(wide == float(2 * i), found[8 * i : 8 * i + 8], total)
    return total[0:4] + total[4:8]


def stacked_rows(ref):
    return jnp.concatenate([ref[i] for i in range(ref.shape[0])], axis=0)


def rank_kernel(*refs):
    *refs, base_ref, sems = refs
    count = (len(refs) - 1) // 2
    far, near, rank_ref = refs[:count], refs[count : 2 * count], refs[-1]
    copies = [pltpu.make_async_copy(far[i], near[i], sems.at[i]) for i in range(count)]
    for copy in copies:
        copy.start()
    for copy in copies:
        copy.wait()
    owner_ref = near[0]
    owners = base_ref.shape[0]
    row = lax.broadcasted_iota(jnp.int32, (LANES, LANES), 0)
    col = lax.broadcasted_iota(jnp.int32, (LANES, LANES), 1)
    before = jnp.where(row < col, 1.0, 0.0).astype(jnp.bfloat16)
    base_ref[...] = jnp.zeros_like(base_ref)

    def ranks(r, carry):
        at = pl.ds(pl.multiple_of(r * LANES, LANES), LANES)
        own = owner_ref[:, at]
        hot = jnp.where(sublane((owners, LANES)) == own, 1.0, 0.0)
        earlier = dot(hot.astype(jnp.bfloat16), before, NN) + base_ref[...]
        rank_ref[:, at] = jnp.sum(hot * earlier, axis=0, keepdims=True)
        base_ref[...] = base_ref[...] + jnp.sum(hot, axis=1, keepdims=True)
        return carry

    lax.fori_loop(0, owner_ref.shape[1] // LANES, ranks, 0, unroll=8)


def pack_kernel(
    owner_ref,
    element_ref,
    coords_ref,
    positions_ref,
    stiff_h_ref,
    stiff_v_ref,
    rank_ref,
    above_ref,
    below_ref,
    out_ref,
    kept_ref,
    wide_ref,
    force_ref,
    acc_ref,
    *,
    capacity,
):
    kept_ref[...] = rank_ref[...]
    units, _, unit = out_ref.shape
    width = acc_ref.shape[1]
    blocks = units * unit // width
    markers = owner_ref.shape[1]
    columns = force_ref.shape[2]
    lines = 4
    step = lines * columns
    membrane_force(positions_ref, above_ref, below_ref, stiff_h_ref, stiff_v_ref, wide_ref, force_ref)
    acc_ref[...] = jnp.zeros_like(acc_ref)

    def route(r, carry):
        at = pl.ds(pl.multiple_of(r * step, step), step)
        slot = owner_ref[:, at].astype(jnp.float32) * float(capacity) + rank_ref[:, at]
        block = jnp.floor((slot + 0.5) * (1.0 / width))
        inside = (slot - block * width - width // 2).astype(jnp.bfloat16)
        force = [
            jnp.concatenate([force_ref[k, pl.ds(lines * r + i, 1), :] for i in range(lines)], axis=1)
            for k in range(3)
        ]
        payload = jnp.concatenate(
            [
                coords_ref[:, at],
                *force,
                element_ref[:, at].astype(jnp.float32) + 1.0,
                jnp.zeros((1, step), jnp.float32),
            ],
            axis=0,
        )
        acc_ref[...] += fold(dot(spread(payload, block, blocks), one_hot(width, inside), NT))
        return carry

    lax.fori_loop(0, markers // step, route, 0)
    for u in range(units):
        h, at = u * unit // width, u * unit % width
        out_ref[u] = acc_ref[8 * h : 8 * h + 8, at : at + unit]


def block_of(got_ref, i, per, capacity):
    count = per * capacity // got_ref.shape[2]
    return jnp.concatenate([got_ref[i * count + j] for j in range(count)], axis=1)


def find_places(got_ref, place_ref, range_ref, hot_ref):
    sources, capacity = place_ref.shape
    groups = range_ref.shape[0]
    row = lax.broadcasted_iota(jnp.int32, (capacity, capacity), 0)
    col = lax.broadcasted_iota(jnp.int32, (capacity, capacity), 1)
    before = jnp.where(row < col, 1.0, 0.0).astype(jnp.bfloat16)
    kind = sublane((groups, capacity)).astype(jnp.float32)
    for s in range(sources):
        group = jnp.floor((block_of(got_ref, s, 1, capacity)[6:7] - 1.0) * (1.0 / GROUP))
        hot_ref[s * groups : (s + 1) * groups, :] = jnp.where(kind == group, 1.0, 0.0)
    earlier = dot(hot_ref[...].astype(jnp.bfloat16), before, NN)
    count = jnp.sum(hot_ref[...], axis=1, keepdims=True)
    total = jnp.zeros((groups, 1), jnp.float32)
    for s in range(sources):
        total = total + count[s * groups : (s + 1) * groups]
    total = jnp.floor((total + (LANES - 1)) * (1.0 / LANES)) * LANES
    start = jnp.zeros((groups, 1), jnp.float32)
    for g in range(groups):
        start = start + jnp.where(sublane((groups, 1)) > g, total[g : g + 1], 0.0)
    base = start + 1.0
    for s in range(sources):
        rows = slice(s * groups, (s + 1) * groups)
        spot = jnp.sum(hot_ref[rows, :] * (earlier[rows] + base), axis=0, keepdims=True) - 1.0
        place_ref[s : s + 1, :] = spot
        base = base + count[rows]
    edge = (lax.broadcasted_iota(jnp.int32, range_ref.shape, 1) * LANES).astype(jnp.float32)
    group = jnp.sum(jnp.where(start + total <= edge, 1.0, 0.0), axis=0, keepdims=True)
    group = jnp.minimum(group, groups - 1.0)
    used = jnp.sum(total, axis=0, keepdims=True) * (1.0 / LANES) + jnp.zeros_like(group)
    range_ref[...] = jnp.where(sublane(range_ref.shape) == 0, group, used).astype(jnp.int32)


def spots(place_ref, i, per):
    spot = jnp.concatenate([place_ref[pl.ds(i * per + j, 1), :] for j in range(per)], axis=1)
    high = jnp.floor(spot * (1.0 / LANES))
    return high, (spot - high * LANES - LANES // 2).astype(jnp.bfloat16)


def batch_of(sources, capacity):
    per = 1
    while per < sources and (per * capacity) % 512 != 0:
        per *= 2
    return per


def sort_markers(got_ref, place_ref, out_ref, acc_ref):
    sources, capacity = place_ref.shape
    chunks = out_ref.shape[0]
    per = batch_of(sources, capacity)
    acc_ref[...] = jnp.zeros_like(acc_ref)

    def gather(i, carry):
        payload = block_of(got_ref, i, per, capacity)
        high, low = spots(place_ref, i, per)
        acc_ref[...] += fold(dot(spread(payload, high, chunks), one_hot(LANES, low), NT))
        return carry

    lax.fori_loop(0, sources // per, gather, 0)
    for h in range(chunks):
        out_ref[h] = acc_ref[8 * h : 8 * h + 8]


def return_samples(place_ref, sampled_ref, out_ref):
    sources, _, capacity = out_ref.shape
    per = batch_of(sources, capacity)
    rows = stacked_rows(sampled_ref)

    def scatter(i, carry):
        high, low = spots(place_ref, i, per)
        total = pick(rows, high, one_hot(LANES, low))
        for j in range(per):
            out_ref[i * per + j] = total[:, j * capacity : (j + 1) * capacity]
        return carry

    lax.fori_loop(0, sources // per, scatter, 0)


def basis_rows(x):
    node = sublane((POINTS, x.shape[1]))
    value = jnp.zeros((POINTS, x.shape[1]), jnp.float32)
    for i in range(POINTS):
        value = jnp.where(node == i, float(SCALE[i]), value)
    for j in range(POINTS):
        value = value * jnp.where(node == j, 1.0, x - float(ABSCISSA[j]))
    return value


def plane_of(payload):
    along_s = basis_rows(payload[1:2])
    along_t = basis_rows(payload[2:3])
    return jnp.concatenate([along_s[b : b + 1] * along_t for b in range(POINTS)], axis=0)


def build_weights(payload, g, weight_ref):
    local = payload[6:7] - (g * GROUP + 1 + GROUP // 2).astype(jnp.float32)
    hot = one_hot(GROUP, local.astype(jnp.bfloat16))
    for i, part in enumerate(split(basis_rows(payload[0:1]))):
        for a in range(POINTS):
            row = jnp.broadcast_to(part[a : a + 1], (16, LANES)).astype(jnp.bfloat16)
            weight_ref[i, a * GROUP : (a + 1) * GROUP, :] = hot * jnp.concatenate([row] * (GROUP // 16), axis=0)


def prepare_kernel(velocity_ref, out_ref):
    groups = out_ref.shape[0]
    half = out_ref.shape[1] // 2
    side = half // 3
    for g in range(groups):
        for k in range(3):
            turned = velocity_ref[k, g * GROUP : (g + 1) * GROUP, :].T
            tile = jnp.concatenate([turned[a * side : (a + 1) * side] for a in range(POINTS)], axis=1)
            high, low = split(tile)
            out_ref[g, k * side : (k + 1) * side, :] = high.astype(jnp.bfloat16)
            out_ref[g, half + k * side : half + (k + 1) * side, :] = low.astype(jnp.bfloat16)


def total_of(wide, narrow):
    half = narrow.shape[0]
    return wide[:half] + wide[half:] + narrow


def pipeline(range_ref, visit, sorted_ref, weight_refs):
    depth = len(weight_refs)
    last = sorted_ref.shape[0] - 1
    for j in range(depth):
        build_weights(sorted_ref[j], range_ref[0, j], weight_refs[j])

    def several(i, carry):
        for j in range(depth):
            c = depth * i + j
            visit(c, range_ref[0, c], weight_refs[j])
            ahead = jnp.minimum(c + depth, last)
            build_weights(sorted_ref[ahead], range_ref[0, ahead], weight_refs[j])
        return carry

    lax.fori_loop(0, (range_ref[1, 0] + (depth - 1)) // depth, several, 0)


def interpolate_kernel(
    got_ref,
    velocity_ref,
    out_ref,
    sorted_ref,
    range_ref,
    place_ref,
    hot_ref,
    acc_ref,
    sampled_ref,
    scalar_ref,
    sem_ref,
    *weight_refs,
):
    find_places(got_ref, place_ref, range_ref, hot_ref)
    spans = pltpu.make_async_copy(range_ref, scalar_ref, sem_ref)
    spans.start()
    sort_markers(got_ref, place_ref, sorted_ref, acc_ref)
    spans.wait()
    sampled_ref[...] = jnp.zeros_like(sampled_ref)

    def visit(c, g, weight_ref):
        half = velocity_ref.shape[1] // 2
        wide = dot(velocity_ref[g], weight_ref[0], NN)
        narrow = dot(velocity_ref[g, 0:half], weight_ref[1], NN)
        total = total_of(wide, narrow)
        plane = plane_of(sorted_ref[c])
        side = plane.shape[0]
        sums = [jnp.sum(plane * total[k * side : (k + 1) * side], axis=0, keepdims=True) for k in range(3)]
        sampled_ref[c] = jnp.concatenate(sums + [jnp.zeros((1, LANES), jnp.float32)], axis=0)

    pipeline(scalar_ref, visit, sorted_ref, weight_refs)
    return_samples(place_ref, sampled_ref, out_ref)


def deposit_kernel(range_ref, sorted_ref, out_ref, sum_ref, *weight_refs):
    sum_ref[...] = jnp.zeros_like(sum_ref)

    def visit(c, g, weight_ref):
        payload = sorted_ref[c]
        plane = plane_of(payload)
        loads = jnp.concatenate([plane * payload[3 + k : 4 + k] for k in range(3)], axis=0)
        left = jnp.concatenate([part.astype(jnp.bfloat16) for part in split(loads)], axis=0)
        wide = dot(left, weight_ref[0], NT)
        narrow = dot(left[: loads.shape[0]], weight_ref[1], NT)
        sum_ref[g] += total_of(wide, narrow)

    pipeline(range_ref, visit, sorted_ref, weight_refs)
    groups, rows, _ = sum_ref.shape
    side = rows // 3
    for g in range(groups):
        for k in range(3):
            turned = sum_ref[g, k * side : (k + 1) * side, :].T
            out_ref[k, g * GROUP : (g + 1) * GROUP, :] = jnp.concatenate(
                [turned[a * GROUP : (a + 1) * GROUP] for a in range(POINTS)], axis=1
            )


def unpack_kernel(owner_ref, rank_ref, arrived_ref, positions_ref, out_ref):
    _, _, capacity = arrived_ref.shape
    columns = positions_ref.shape[2]
    lines = 4
    step = lines * columns
    rows = stacked_rows(arrived_ref)

    def chunk(r, carry):
        at = pl.ds(pl.multiple_of(r * step, step), step)
        rank = (rank_ref[:, at] - capacity // 2).astype(jnp.bfloat16)
        moved = pick(rows, owner_ref[:, at].astype(jnp.float32), one_hot(capacity, rank))
        for k in range(3):
            for i in range(lines):
                row = pl.ds(lines * r + i, 1)
                part = moved[k : k + 1, i * columns : (i + 1) * columns]
                out_ref[k, row, :] = positions_ref[k, row, :] + time_step * part
        return carry

    lax.fori_loop(0, owner_ref.shape[1] // step, chunk, 0)


def near(*arrays):
    return [pltpu.with_memory_space_constraint(x, pltpu.VMEM) for x in arrays]


def away(*arrays):
    return [pltpu.with_memory_space_constraint(x, pltpu.HBM) for x in arrays]


def exchange(x):
    return lax.all_to_all(x, AXES, 0, 0, tiled=True)


def local(velocity, positions, stiff_h, stiff_v, marker_owner, marker_element, marker_coords):
    devices = lax.axis_size(AXES)
    markers = marker_owner.shape[0]
    capacity = 3 * markers // (2 * devices)
    slots = devices * capacity
    elements = velocity.shape[1]
    groups = elements // GROUP
    side = velocity.shape[2] // POINTS
    f32 = jnp.float32

    above, below = halo(positions, stiff_v)
    owner = marker_owner.reshape(1, markers)
    element = marker_element.reshape(1, markers)
    hbm = pl.BlockSpec(memory_space=pltpu.HBM)
    far = (owner, element, marker_coords, positions, stiff_h, stiff_v)
    *close, rank = pl.pallas_call(
        rank_kernel,
        out_shape=[pltpu.VMEM(x.shape, x.dtype) for x in far] + [pltpu.VMEM((1, markers), f32)],
        in_specs=[hbm] * len(far),
        scratch_shapes=[pltpu.VMEM((devices, 1), f32), pltpu.SemaphoreType.DMA((len(far),))],
        compiler_params=SMALL,
        name="rank",
    )(*away(*far))
    rows, columns = stiff_h.shape
    whole = capacity % 128 == 0 and slots % LANES == 0
    unit = 128 if whole else capacity
    width = LANES if whole else capacity
    outgoing, kept = pl.pallas_call(
        functools.partial(pack_kernel, capacity=capacity),
        out_shape=(
            jax.ShapeDtypeStruct((slots // unit, 8, unit), f32),
            jax.ShapeDtypeStruct((1, markers), f32),
        ),
        scratch_shapes=[
            pltpu.VMEM((4, rows + 16, columns), f32),
            pltpu.VMEM((3, rows, columns), f32),
            pltpu.VMEM((slots // width * 8, width), f32),
        ],
        compiler_params=SMALL,
        name="pack",
    )(*near(*close, rank, above, below))
    got = exchange(outgoing)
    table = pl.pallas_call(
        prepare_kernel,
        out_shape=pltpu.VMEM((groups, 6 * side, POINTS * GROUP), jnp.bfloat16),
        compiler_params=SMALL,
        name="prepare",
    )(*near(velocity))
    chunks = slots // LANES + groups
    weights = pltpu.VMEM((2, POINTS * GROUP, LANES), jnp.bfloat16)
    returning, ordered, spans = pl.pallas_call(
        interpolate_kernel,
        out_shape=(
            pltpu.VMEM((devices, 4, capacity), f32),
            pltpu.VMEM((chunks, 8, LANES), f32),
            jax.ShapeDtypeStruct((groups, 128), jnp.int32),
        ),
        scratch_shapes=[
            pltpu.VMEM((devices, capacity), f32),
            pltpu.VMEM((devices * groups, capacity), f32),
            pltpu.VMEM((chunks * 8, LANES), f32),
            pltpu.VMEM((chunks, 4, LANES), f32),
            pltpu.SMEM((groups, 128), jnp.int32),
            pltpu.SemaphoreType.DMA,
            *[weights] * DEPTH,
        ],
        compiler_params=SMALL,
        name="interpolate",
    )(*near(got, table))
    arrived = exchange(returning)
    node_forces = pl.pallas_call(
        deposit_kernel,
        out_shape=jax.ShapeDtypeStruct(velocity.shape, f32),
        in_specs=[pl.BlockSpec(memory_space=pltpu.SMEM), pl.BlockSpec(memory_space=pltpu.VMEM)],
        scratch_shapes=[pltpu.VMEM((groups, 3 * side, POINTS * GROUP), f32)] + [weights] * DEPTH,
        compiler_params=SMALL,
        name="deposit",
    )(spans, *near(ordered))
    moved = pl.pallas_call(
        unpack_kernel,
        out_shape=jax.ShapeDtypeStruct(positions.shape, f32),
        compiler_params=SMALL,
        name="unpack",
    )(*near(owner, kept, arrived, positions))
    return moved, node_forces


def solution(mesh):
    return jax.shard_map(
        local,
        mesh=mesh,
        in_specs=(
            P(None, AXES, None),
            P(None, AXES, None),
            P(AXES, None),
            P(AXES, None),
            P(AXES, None),
            P(AXES),
            P(None, AXES),
        ),
        out_specs=(P(None, AXES, None), P(None, AXES, None)),
        check_vma=False,
    )
```

```python
import functools

import jax
import jax.numpy as jnp
import numpy as np
from jax import lax
from jax.experimental import pallas as pl
from jax.experimental.pallas import tpu as pltpu
from jax.sharding import PartitionSpec as P

POINTS = 8
AXES = ("gx", "gy")
SMALL = pltpu.CompilerParams(vmem_limit_bytes=20 * 1024 * 1024)
LANES = 256
GROUP = 32
DEPTH = 4

bend_modulus = 0.05
time_step = 0.5

ABSCISSA = -np.cos(np.pi * np.arange(POINTS) / (POINTS - 1))
SCALE = np.array(
    [1.0 / np.prod([ABSCISSA[i] - ABSCISSA[j] for j in range(POINTS) if j != i]) for i in range(POINTS)]
)

NN = (((1,), (0,)), ((), ()))
NT = (((1,), (1,)), ((), ()))


def dot(a, b, dims):
    return lax.dot_general(a, b, dims, preferred_element_type=jnp.float32)


def split(x):
    high = x.astype(jnp.bfloat16).astype(jnp.float32)
    return high, x - high


def sublane(shape):
    return lax.broadcasted_iota(jnp.int32, shape, 0)


def halo(positions, stiff_v):
    count = lax.axis_size(AXES)
    stacked = jnp.concatenate([positions, stiff_v[None]], axis=0)
    tail = stacked[:, -2:]
    head = stacked[:, :2]
    above = lax.ppermute(tail, AXES, [(i, (i + 1) % count) for i in range(count)])
    below = lax.ppermute(head, AXES, [((i + 1) % count, i) for i in range(count)])
    return above, below


def around(x, rows, cols):
    if rows:
        return pltpu.roll(x, rows % x.shape[0], 0)
    return pltpu.roll(x, cols % x.shape[1], 1)


def surface_laplacian(x):
    return around(x, -1, 0) + around(x, 1, 0) + around(x, 0, 1) + around(x, 0, -1) - 4.0 * x


def membrane_force(positions_ref, above_ref, below_ref, stiff_h_ref, stiff_v_ref, wide_ref, force_ref):
    rows = stiff_h_ref.shape[0]
    inner = slice(8, 8 + rows)
    stiff_h = stiff_h_ref[...]
    stiff_v = stiff_v_ref[...]
    wide_ref[3, inner, :] = stiff_v
    wide_ref[3, 7:8, :] = above_ref[3, 1:2, :]
    stiff_before = wide_ref[3, 7 : 7 + rows, :]
    for k in range(3):
        wide_ref[k, inner, :] = positions_ref[k]
        wide_ref[k, 6:8, :] = above_ref[k]
        wide_ref[k, 8 + rows : 10 + rows, :] = below_ref[k]
        wide = wide_ref[k]
        middle = wide[inner]
        pulling = (
            stiff_h * (around(middle, 0, -1) - middle)
            + around(stiff_h, 0, 1) * (around(middle, 0, 1) - middle)
            + stiff_v * (around(wide, -1, 0)[inner] - middle)
            + stiff_before * (around(wide, 1, 0)[inner] - middle)
        )
        bending = surface_laplacian(surface_laplacian(wide))[inner]
        force_ref[k] = pulling - bend_modulus * bending


def one_hot(count, centred):
    shape = (count, centred.shape[1])
    row = (sublane(shape) - count // 2).astype(jnp.bfloat16)
    return jnp.where(row == centred, jnp.bfloat16(1), jnp.bfloat16(0))


def spread(payload, label, count):
    wide = jnp.broadcast_to(label, (16, label.shape[1]))
    wide = (wide - (sublane(wide.shape) // 8).astype(jnp.float32)).astype(jnp.bfloat16)
    masks = [wide == jnp.bfloat16(2 * i) for i in range(count // 2)]
    sides = []
    for part in split(payload):
        twice = jnp.concatenate([part, part], axis=0).astype(jnp.bfloat16)
        sides.append(jnp.concatenate([jnp.where(mask, twice, jnp.bfloat16(0)) for mask in masks], axis=0))
    return jnp.concatenate(sides, axis=0)


def fold(x):
    half = x.shape[0] // 2
    return x[:half] + x[half:]


def pick(rows, label, right):
    parts = [part.astype(jnp.bfloat16) for part in split(rows)]
    if rows.shape[1] % 128 == 0:
        found = dot(jnp.concatenate(parts, axis=1), jnp.concatenate([right, right], axis=0), NN)
    else:
        found = dot(parts[0], right, NN) + dot(parts[1], right, NN)
    wide = jnp.broadcast_to(label, (8, label.shape[1]))
    wide = wide - (sublane(wide.shape) // 4).astype(jnp.float32)
    total = jnp.zeros(wide.shape, jnp.float32)
    for i in range(rows.shape[0] // 8):
        total = jnp.where(wide == float(2 * i), found[8 * i : 8 * i + 8], total)
    return total[0:4] + total[4:8]


def stacked_rows(ref):
    return jnp.concatenate([ref[i] for i in range(ref.shape[0])], axis=0)


def rank_kernel(*refs):
    *refs, base_ref, sems = refs
    count = (len(refs) - 1) // 2
    far, near, rank_ref = refs[:count], refs[count : 2 * count], refs[-1]
    copies = [pltpu.make_async_copy(far[i], near[i], sems.at[i]) for i in range(count)]
    for copy in copies:
        copy.start()
    for copy in copies:
        copy.wait()
    owner_ref = near[0]
    owners = base_ref.shape[0]
    row = lax.broadcasted_iota(jnp.int32, (LANES, LANES), 0)
    col = lax.broadcasted_iota(jnp.int32, (LANES, LANES), 1)
    before = jnp.where(row < col, 1.0, 0.0).astype(jnp.bfloat16)
    base_ref[...] = jnp.zeros_like(base_ref)

    def ranks(r, carry):
        at = pl.ds(pl.multiple_of(r * LANES, LANES), LANES)
        own = owner_ref[:, at]
        hot = jnp.where(sublane((owners, LANES)) == own, 1.0, 0.0)
        earlier = dot(hot.astype(jnp.bfloat16), before, NN) + base_ref[...]
        rank_ref[:, at] = jnp.sum(hot * earlier, axis=0, keepdims=True)
        base_ref[...] = base_ref[...] + jnp.sum(hot, axis=1, keepdims=True)
        return carry

    lax.fori_loop(0, owner_ref.shape[1] // LANES, ranks, 0, unroll=8)


def pack_kernel(
    owner_ref,
    element_ref,
    coords_ref,
    positions_ref,
    stiff_h_ref,
    stiff_v_ref,
    rank_ref,
    above_ref,
    below_ref,
    out_ref,
    kept_ref,
    wide_ref,
    force_ref,
    acc_ref,
    sem_ref,
    *,
    capacity,
):
    keep = pltpu.make_async_copy(rank_ref, kept_ref, sem_ref)
    keep.start()
    units, _, unit = out_ref.shape
    width = acc_ref.shape[1]
    blocks = units * unit // width
    markers = owner_ref.shape[1]
    columns = force_ref.shape[2]
    lines = 4
    step = lines * columns
    membrane_force(positions_ref, above_ref, below_ref, stiff_h_ref, stiff_v_ref, wide_ref, force_ref)
    acc_ref[...] = jnp.zeros_like(acc_ref)

    def route(r, carry):
        at = pl.ds(pl.multiple_of(r * step, step), step)
        slot = owner_ref[:, at].astype(jnp.float32) * float(capacity) + rank_ref[:, at]
        block = jnp.floor((slot + 0.5) * (1.0 / width))
        inside = (slot - block * width - width // 2).astype(jnp.bfloat16)
        force = [
            jnp.concatenate([force_ref[k, pl.ds(lines * r + i, 1), :] for i in range(lines)], axis=1)
            for k in range(3)
        ]
        payload = jnp.concatenate(
            [
                coords_ref[:, at],
                *force,
                element_ref[:, at].astype(jnp.float32) + 1.0,
                jnp.zeros((1, step), jnp.float32),
            ],
            axis=0,
        )
        acc_ref[...] += fold(dot(spread(payload, block, blocks), one_hot(width, inside), NT))
        return carry

    lax.fori_loop(0, markers // step, route, 0, unroll=8)
    for u in range(units):
        h, at = u * unit // width, u * unit % width
        out_ref[u] = acc_ref[8 * h : 8 * h + 8, at : at + unit]
    keep.wait()


def block_of(got_ref, i, per, capacity):
    count = per * capacity // got_ref.shape[2]
    return jnp.concatenate([got_ref[i * count + j] for j in range(count)], axis=1)


def find_places(got_ref, place_ref, range_ref, hot_ref):
    sources, capacity = place_ref.shape
    groups = range_ref.shape[0]
    row = lax.broadcasted_iota(jnp.int32, (capacity, capacity), 0)
    col = lax.broadcasted_iota(jnp.int32, (capacity, capacity), 1)
    before = jnp.where(row < col, 1.0, 0.0).astype(jnp.bfloat16)
    kind = sublane((groups, capacity)).astype(jnp.float32)
    for s in range(sources):
        group = jnp.floor((block_of(got_ref, s, 1, capacity)[6:7] - 1.0) * (1.0 / GROUP))
        hot_ref[s * groups : (s + 1) * groups, :] = jnp.where(kind == group, 1.0, 0.0)
    earlier = dot(hot_ref[...].astype(jnp.bfloat16), before, NN)
    count = jnp.sum(hot_ref[...], axis=1, keepdims=True)
    total = jnp.zeros((groups, 1), jnp.float32)
    for s in range(sources):
        total = total + count[s * groups : (s + 1) * groups]
    total = jnp.floor((total + (LANES - 1)) * (1.0 / LANES)) * LANES
    start = jnp.zeros((groups, 1), jnp.float32)
    for g in range(groups):
        start = start + jnp.where(sublane((groups, 1)) > g, total[g : g + 1], 0.0)
    base = start + 1.0
    for s in range(sources):
        rows = slice(s * groups, (s + 1) * groups)
        spot = jnp.sum(hot_ref[rows, :] * (earlier[rows] + base), axis=0, keepdims=True) - 1.0
        place_ref[s : s + 1, :] = spot
        base = base + count[rows]
    edge = (lax.broadcasted_iota(jnp.int32, range_ref.shape, 1) * LANES).astype(jnp.float32)
    group = jnp.sum(jnp.where(start + total <= edge, 1.0, 0.0), axis=0, keepdims=True)
    group = jnp.minimum(group, groups - 1.0)
    used = jnp.sum(total, axis=0, keepdims=True) * (1.0 / LANES) + jnp.zeros_like(group)
    range_ref[...] = jnp.where(sublane(range_ref.shape) == 0, group, used).astype(jnp.int32)


def spots(place_ref, i, per):
    spot = jnp.concatenate([place_ref[pl.ds(i * per + j, 1), :] for j in range(per)], axis=1)
    high = jnp.floor(spot * (1.0 / LANES))
    return high, (spot - high * LANES - LANES // 2).astype(jnp.bfloat16)


def batch_of(sources, capacity):
    per = 1
    while per < sources and (per * capacity) % 512 != 0:
        per *= 2
    return per


def sort_markers(got_ref, place_ref, out_ref, acc_ref):
    sources, capacity = place_ref.shape
    chunks = out_ref.shape[0]
    per = batch_of(sources, capacity)
    acc_ref[...] = jnp.zeros_like(acc_ref)

    def gather(i, carry):
        payload = block_of(got_ref, i, per, capacity)
        high, low = spots(place_ref, i, per)
        acc_ref[...] += fold(dot(spread(payload, high, chunks), one_hot(LANES, low), NT))
        return carry

    lax.fori_loop(0, sources // per, gather, 0, unroll=4)
    for h in range(chunks):
        out_ref[h] = acc_ref[8 * h : 8 * h + 8]


def return_samples(place_ref, sampled_ref, out_ref):
    sources, _, capacity = out_ref.shape
    per = batch_of(sources, capacity)
    rows = stacked_rows(sampled_ref)

    def scatter(i, carry):
        high, low = spots(place_ref, i, per)
        total = pick(rows, high, one_hot(LANES, low))
        for j in range(per):
            out_ref[i * per + j] = total[:, j * capacity : (j + 1) * capacity]
        return carry

    lax.fori_loop(0, sources // per, scatter, 0, unroll=4)


def basis_rows(x):
    node = sublane((POINTS, x.shape[1]))
    value = jnp.zeros((POINTS, x.shape[1]), jnp.float32)
    for i in range(POINTS):
        value = jnp.where(node == i, float(SCALE[i]), value)
    for j in range(POINTS):
        value = value * jnp.where(node == j, 1.0, x - float(ABSCISSA[j]))
    return value


def plane_of(payload):
    along_s = basis_rows(payload[1:2])
    along_t = basis_rows(payload[2:3])
    return jnp.concatenate([along_s[b : b + 1] * along_t for b in range(POINTS)], axis=0)


def build_weights(payload, g, weight_ref):
    local = payload[6:7] - (g * GROUP + 1 + GROUP // 2).astype(jnp.float32)
    hot = one_hot(GROUP, local.astype(jnp.bfloat16))
    for i, part in enumerate(split(basis_rows(payload[0:1]))):
        for a in range(POINTS):
            row = jnp.broadcast_to(part[a : a + 1], (8, LANES))
            row = jnp.concatenate([row, row], axis=0).astype(jnp.bfloat16)
            for e in range(0, GROUP, 16):
                weight_ref[i, a * GROUP + e : a * GROUP + e + 16, :] = hot[e : e + 16] * row


def prepare_kernel(velocity_ref, out_ref):
    groups = out_ref.shape[0]
    half = out_ref.shape[1] // 2
    side = half // 3
    for g in range(groups):
        for k in range(3):
            turned = velocity_ref[k, g * GROUP : (g + 1) * GROUP, :].T
            tile = jnp.concatenate([turned[a * side : (a + 1) * side] for a in range(POINTS)], axis=1)
            high, low = split(tile)
            out_ref[g, k * side : (k + 1) * side, :] = high.astype(jnp.bfloat16)
            out_ref[g, half + k * side : half + (k + 1) * side, :] = low.astype(jnp.bfloat16)


def product(left, weight_ref, dims, swap):
    half = left.shape[0] // 2
    if swap:
        narrow = dot(left[:half], weight_ref[1], dims)
        wide = dot(left, weight_ref[0], dims)
    else:
        wide = dot(left, weight_ref[0], dims)
        narrow = dot(left[:half], weight_ref[1], dims)
    return wide[:half] + wide[half:] + narrow


def pipeline(range_ref, visit, sorted_ref, weight_refs):
    depth = len(weight_refs)
    last = sorted_ref.shape[0] - 1
    for j in range(depth):
        build_weights(sorted_ref[j], range_ref[0, j], weight_refs[j])

    def several(i, carry):
        for j in range(depth):
            c = depth * i + j
            visit(c, range_ref[0, c], weight_refs[j], j % 2 == 1)
            ahead = jnp.minimum(c + depth, last)
            build_weights(sorted_ref[ahead], range_ref[0, ahead], weight_refs[j])
        return carry

    lax.fori_loop(0, (range_ref[1, 0] + (depth - 1)) // depth, several, 0)


def interpolate_kernel(
    got_ref,
    velocity_ref,
    out_ref,
    sorted_ref,
    range_ref,
    place_ref,
    hot_ref,
    acc_ref,
    sampled_ref,
    scalar_ref,
    sem_ref,
    *weight_refs,
):
    find_places(got_ref, place_ref, range_ref, hot_ref)
    spans = pltpu.make_async_copy(range_ref, scalar_ref, sem_ref)
    spans.start()
    sort_markers(got_ref, place_ref, sorted_ref, acc_ref)
    spans.wait()
    sampled_ref[...] = jnp.zeros_like(sampled_ref)

    def visit(c, g, weight_ref, swap):
        total = product(velocity_ref[g], weight_ref, NN, swap)
        plane = plane_of(sorted_ref[c])
        side = plane.shape[0]
        sums = [jnp.sum(plane * total[k * side : (k + 1) * side], axis=0, keepdims=True) for k in range(3)]
        sampled_ref[c] = jnp.concatenate(sums + [jnp.zeros((1, LANES), jnp.float32)], axis=0)

    pipeline(scalar_ref, visit, sorted_ref, weight_refs)
    return_samples(place_ref, sampled_ref, out_ref)


def deposit_kernel(range_ref, sorted_ref, out_ref, sum_ref, *weight_refs):
    sum_ref[...] = jnp.zeros_like(sum_ref)

    def visit(c, g, weight_ref, swap):
        payload = sorted_ref[c]
        plane = plane_of(payload)
        loads = jnp.concatenate([plane * payload[3 + k : 4 + k] for k in range(3)], axis=0)
        left = jnp.concatenate([part.astype(jnp.bfloat16) for part in split(loads)], axis=0)
        sum_ref[g] += product(left, weight_ref, NT, swap)

    pipeline(range_ref, visit, sorted_ref, weight_refs)
    groups, rows, _ = sum_ref.shape
    side = rows // 3
    for g in range(groups):
        for k in range(3):
            turned = sum_ref[g, k * side : (k + 1) * side, :].T
            out_ref[k, g * GROUP : (g + 1) * GROUP, :] = jnp.concatenate(
                [turned[a * GROUP : (a + 1) * GROUP] for a in range(POINTS)], axis=1
            )


def unpack_kernel(owner_ref, rank_ref, arrived_ref, positions_ref, out_ref):
    _, _, capacity = arrived_ref.shape
    columns = positions_ref.shape[2]
    lines = 4
    step = lines * columns
    rows = stacked_rows(arrived_ref)

    def chunk(r, carry):
        at = pl.ds(pl.multiple_of(r * step, step), step)
        rank = (rank_ref[:, at] - capacity // 2).astype(jnp.bfloat16)
        moved = pick(rows, owner_ref[:, at].astype(jnp.float32), one_hot(capacity, rank))
        for k in range(3):
            for i in range(lines):
                row = pl.ds(lines * r + i, 1)
                part = moved[k : k + 1, i * columns : (i + 1) * columns]
                out_ref[k, row, :] = positions_ref[k, row, :] + time_step * part
        return carry

    lax.fori_loop(0, owner_ref.shape[1] // step, chunk, 0, unroll=8)


def near(*arrays):
    return [pltpu.with_memory_space_constraint(x, pltpu.VMEM) for x in arrays]


def away(*arrays):
    return [pltpu.with_memory_space_constraint(x, pltpu.HBM) for x in arrays]


def exchange(x):
    return lax.all_to_all(x, AXES, 0, 0, tiled=True)


def local(velocity, positions, stiff_h, stiff_v, marker_owner, marker_element, marker_coords):
    devices = lax.axis_size(AXES)
    markers = marker_owner.shape[0]
    capacity = 3 * markers // (2 * devices)
    slots = devices * capacity
    elements = velocity.shape[1]
    groups = elements // GROUP
    side = velocity.shape[2] // POINTS
    f32 = jnp.float32

    above, below = halo(positions, stiff_v)
    owner = marker_owner.reshape(1, markers)
    element = marker_element.reshape(1, markers)
    hbm = pl.BlockSpec(memory_space=pltpu.HBM)
    far = (owner, element, marker_coords, positions, stiff_h, stiff_v)
    *close, rank = pl.pallas_call(
        rank_kernel,
        out_shape=[pltpu.VMEM(x.shape, x.dtype) for x in far] + [pltpu.VMEM((1, markers), f32)],
        in_specs=[hbm] * len(far),
        scratch_shapes=[pltpu.VMEM((devices, 1), f32), pltpu.SemaphoreType.DMA((len(far),))],
        compiler_params=SMALL,
        name="rank",
    )(*away(*far))
    rows, columns = stiff_h.shape
    whole = capacity % 128 == 0 and slots % LANES == 0
    unit = 128 if whole else capacity
    width = LANES if whole else capacity
    outgoing, kept = pl.pallas_call(
        functools.partial(pack_kernel, capacity=capacity),
        out_shape=(
            jax.ShapeDtypeStruct((slots // unit, 8, unit), f32),
            pltpu.HBM((1, markers), f32),
        ),
        scratch_shapes=[
            pltpu.VMEM((4, rows + 16, columns), f32),
            pltpu.VMEM((3, rows, columns), f32),
            pltpu.VMEM((slots // width * 8, width), f32),
            pltpu.SemaphoreType.DMA,
        ],
        compiler_params=SMALL,
        name="pack",
    )(*near(*close, rank, above, below))
    got = exchange(outgoing)
    table = pl.pallas_call(
        prepare_kernel,
        out_shape=pltpu.VMEM((groups, 6 * side, POINTS * GROUP), jnp.bfloat16),
        compiler_params=SMALL,
        name="prepare",
    )(*near(velocity))
    chunks = slots // LANES + groups
    weights = pltpu.VMEM((2, POINTS * GROUP, LANES), jnp.bfloat16)
    returning, ordered, spans = pl.pallas_call(
        interpolate_kernel,
        out_shape=(
            pltpu.VMEM((devices, 4, capacity), f32),
            pltpu.VMEM((chunks, 8, LANES), f32),
            jax.ShapeDtypeStruct((groups, 128), jnp.int32),
        ),
        scratch_shapes=[
            pltpu.VMEM((devices, capacity), f32),
            pltpu.VMEM((devices * groups, capacity), f32),
            pltpu.VMEM((chunks * 8, LANES), f32),
            pltpu.VMEM((chunks, 4, LANES), f32),
            pltpu.SMEM((groups, 128), jnp.int32),
            pltpu.SemaphoreType.DMA,
            *[weights] * DEPTH,
        ],
        compiler_params=SMALL,
        name="interpolate",
    )(*near(got, table))
    arrived = exchange(returning)
    node_forces = pl.pallas_call(
        deposit_kernel,
        out_shape=jax.ShapeDtypeStruct(velocity.shape, f32),
        in_specs=[pl.BlockSpec(memory_space=pltpu.SMEM), pl.BlockSpec(memory_space=pltpu.VMEM)],
        scratch_shapes=[pltpu.VMEM((groups, 3 * side, POINTS * GROUP), f32)] + [weights] * DEPTH,
        compiler_params=SMALL,
        name="deposit",
    )(spans, *near(ordered))
    moved = pl.pallas_call(
        unpack_kernel,
        out_shape=jax.ShapeDtypeStruct(positions.shape, f32),
        compiler_params=SMALL,
        name="unpack",
    )(*near(owner, kept, arrived, positions))
    return moved, node_forces


def solution(mesh):
    return jax.shard_map(
        local,
        mesh=mesh,
        in_specs=(
            P(None, AXES, None),
            P(None, AXES, None),
            P(AXES, None),
            P(AXES, None),
            P(AXES, None),
            P(AXES),
            P(None, AXES),
        ),
        out_specs=(P(None, AXES, None), P(None, AXES, None)),
        check_vma=False,
    )
```
